32 devices in a mesh: grp: 2 (over core), tile: 16 (over z, y, x).
Axes of the slice: x: 2, y: 2, z: 4, core: 2. Of those that a mesh axis runs over, the one named last changes fastest.
Arguments:
- attn_input: bfloat16 [2048, 4096], P(('grp', 'tile')), may hold values from -9 to 9
- mlp_input: bfloat16 [2048, 4096], P(('grp', 'tile')), may hold values from -9 to 9
Outputs:
- hess_attn: float32 [16, 1024, 1024], P('tile', 'grp')
- hess_mlp: float32 [16, 1024, 1024], P('tile', 'grp')
The draws below stay inside these ranges and needn't reach their ends.
All inputs are finite; a program needn't handle non-finite values.
Results may differ from the reference program's by a relative error of at most 0.0003.
Values may be sent and summed in bfloat16 or wider, within the bound.
A program may use at most 192 MiB of HBM per device.

```python
import jax
import jax.numpy as jnp
from jax import lax

W = 4096
ROWB = 4
TOKENS = 2048
COLB = 4
RT = 1024
CT = 1024


def block_levels(rng, dims, pieces, least, largest):
    level = 1.0
    for axis_at, shards_of in pieces:
        draws = jax.random.uniform(jax.random.fold_in(jax.random.fold_in(rng, 6), axis_at), (shards_of,), jnp.float32, least / len(pieces), largest / len(pieces))
        level = level * jnp.repeat(jnp.exp(draws), dims[axis_at] // shards_of).reshape((-1,) + (1,) * (len(dims) - 1 - axis_at))
    return level


def gaussian(key, dims, width, reach, cuts=(), dtype=jnp.bfloat16):
    array = jax.random.normal(key, dims, jnp.float32) * width
    if len(cuts) > 0:
        array = block_levels(key, dims, cuts, -0.22, 0.18) * array
    return jnp.clip(array, min=-reach, max=reach).astype(dtype)


def setup_inputs(seed: int = 0) -> dict:
    key_of = jax.random.split(jax.random.key(seed), 3)
    return {
        "attn_input": gaussian(key_of[0], (TOKENS, W), 1.5, 9.0, ((0, 32),)),
        "mlp_input": gaussian(key_of[1], (TOKENS, W), 1.5, 9.0, ((0, 32),)),
    }


def hessian_tiles(inputs):
    widened = inputs.astype(jnp.float32)
    gram_full = jnp.dot(widened.T, widened, precision=lax.Precision.HIGHEST)
    gram_full = gram_full * (2.0 / TOKENS)
    tiled = gram_full.reshape(ROWB, RT, COLB, CT).transpose(0, 2, 1, 3)
    return tiled.reshape(ROWB * COLB, RT, CT)


def reference(attn_input, mlp_input):
    return (hessian_tiles(attn_input), hessian_tiles(mlp_input))
```

```python
import jax
import jax.numpy as jnp
from jax import lax
from jax.experimental import pallas as pl
from jax.experimental.pallas import tpu as pltpu
from jax.sharding import PartitionSpec as P

ROWB = 4
TOKB = 32
MESH = pl.DeviceIdType.MESH
LINE = 0
RING = 1
AHEAD = 3
CROSS_AT = 2
CROSS_LATE = 9
CROSS_WAIT = 5
FAR_LAG = 1
SPAN_LAG = 2
MUL_LAG = 4
VMEM_LIMIT = 48 * 1024 * 1024
IN_SPACE = pltpu.HBM


def tile_first(inputs, tile_count):
    tok_rows, feat_width = inputs.shape
    col_blocks = tile_count // ROWB
    row_width = feat_width // ROWB
    col_width = feat_width // col_blocks

    def accumulate(turn_idx, partial_value):
        tok_block = lax.dynamic_slice_in_dim(inputs, turn_idx * TOKB, TOKB, 0)
        row_parts = tok_block.reshape(TOKB, ROWB, row_width).transpose(1, 0, 2)
        row_send = jnp.repeat(row_parts, col_blocks, axis=0)
        col_parts = tok_block.reshape(TOKB, col_blocks, col_width).transpose(1, 0, 2)
        col_send = jnp.tile(col_parts, (ROWB, 1, 1))
        rows_in, cols_in = (
            lax.all_to_all(row_send, "tile", split_axis=0, concat_axis=0, tiled=True),
            lax.all_to_all(col_send, "tile", split_axis=0, concat_axis=0, tiled=True),
        )
        rows_flat = rows_in.reshape(tile_count * TOKB, row_width)
        cols_flat = cols_in.reshape(tile_count * TOKB, col_width)
        return partial_value + lax.dot_general(
            rows_flat, cols_flat, (((0,), (0,)), ((), ())), preferred_element_type=jnp.float32
        )

    partial_value = lax.fori_loop(
        0, tok_rows // TOKB, accumulate, jnp.zeros((row_width, col_width), jnp.float32)
    )
    shares = lax.psum_scatter(partial_value, "grp", scatter_dimension=0, tiled=True)
    return shares[None]


def hessian_share(inputs):
    tile_count = lax.axis_size("tile")
    group_count = lax.axis_size("grp")
    norm_factor = 2.0 / (inputs.shape[0] * tile_count * group_count)
    shares = tile_first(inputs, tile_count)
    return shares * norm_factor


def ring_place(member):
    return member + (member // 2) * (1 - 2 * (member % 2))


def piece_of(home, turn):
    near = home + 1 - 2 * (home % 2)
    far = (home + 2) % ROWB
    return jnp.where(turn == 0, home, jnp.where(turn == 1, near, jnp.where(turn == 2, far, ROWB - 1 - home)))


def kernel(xa, xm, out_a, out_m, xbuf, cbuf, rbuf, own_sem, ld_sem, x_recv, c_recv, r_recv, s1_send, x_send, d_send, z_send):
    lines = planes = ROWB
    group = 4 * planes
    side = group * (lines - 1)
    total = group * (2 * lines - 1)
    g = lax.axis_index("grp")
    t = lax.axis_index("tile")
    z, p = t // planes, t % planes
    tok, _ = xa.shape
    ct = cbuf.shape[-1]
    rh = ct // 2
    xs = (xa, xm)
    outs = (out_a, out_m)
    is_line = g == LINE
    line_half = pl.ds(LINE * rh, rh)
    my_half = pl.ds(pl.multiple_of(g * rh, rh), rh)

    fwd = (ring_place(p) - ring_place(z) + planes) % planes
    bwd = (planes - fwd) % planes
    is_root = fwd == 0
    ring_fwd = ring_place((ring_place(p) + 1) % planes)
    ring_bwd = ring_place((ring_place(p) + planes - 1) % planes)
    fwd_is_near = ring_fwd == piece_of(p, 1)

    low_side = z < lines // 2
    upper = z // (lines // 2)
    end_z = upper * (lines - 1)
    at_end = z == end_z
    place = p + upper * (planes - 1 - 2 * p)
    beside = 1 + upper * (lines - 3)
    across = end_z + beside - z
    end_step = 2 * upper - 1
    toward = jnp.where(low_side, group, group + side)
    away = group + group + side - toward

    def crosses(turn):
        return (turn >= 1) & (turn <= 2) & ((place == 0) | (place == turn))

    def comes_late(turn, dist):
        return at_end & (dist == 1) & (turn >= 1) & (turn <= 2) & (place == turn)

    slot_late = at_end & ((place == 1) | (place == 2))

    def near_of(turn):
        return turn + 1 - 2 * (turn % 2)

    def far_of(turn):
        return (turn + 2) % planes

    def local_turn(turn):
        return jnp.where(
            is_root, turn, jnp.where(
                z == piece_of(p, 1), near_of(turn), jnp.where(z == piece_of(p, 2), far_of(turn), planes - 1 - turn)))

    def next_turn(turn, way):
        return jnp.where(fwd_is_near == (way == 0), near_of(turn), far_of(turn))

    def chip(zz, pp, gg):
        return (gg, zz * planes + pp)

    pair = chip(z, p, 1 - g)
    ring_next = [chip(z, ring_fwd, RING), chip(z, ring_bwd, RING)]

    def landed(ref, sem):
        pltpu.make_async_copy(ref, ref, sem).wait()

    def cols(block):
        return pl.ds(pl.multiple_of(block * ct, ct), ct)

    def own_index(a, turn, gg):
        return 2 * planes * a + 2 * turn + gg

    def loan_index(a, turn, gg):
        return (2 * gg + a) * (planes - 1) + turn - 1

    def load_own(a):
        return pltpu.make_async_copy(xs[a].at[:, cols(p)], cbuf.at[own_index(a, 0, g)], own_sem.at[a])

    def load(a, turn):
        return pltpu.make_async_copy(
            xs[a].at[:, cols(piece_of(p, turn))], xbuf.at[loan_index(a, turn, g)], ld_sem.at[a, turn - 1])

    for a in range(2):
        load_own(a).start()
    for turn in range(1, planes):
        for a in range(2):
            load(a, turn).start()

    barrier = pltpu.get_barrier_semaphore()

    def greet(device):
        pl.semaphore_signal(barrier, inc=1, device_id=device, device_id_type=MESH)

    greet(pair)

    @pl.when(is_line)
    def _():
        for turn in range(1, planes):
            for gg in range(2):
                greet(chip(z, piece_of(p, turn), gg))
        for turn in range(1, 3):
            @pl.when(crosses(turn))
            def _():
                greet(chip(across, piece_of(p, turn), LINE))

        @pl.when(z > 0)
        def _():
            greet(chip(z - 1, p, LINE))

        @pl.when(z < lines - 1)
        def _():
            greet(chip(z + 1, p, LINE))

        pl.semaphore_wait(
            barrier, planes + jnp.where(z > 0, 1, 0) + jnp.where(z < lines - 1, 1, 0)
            + jnp.where(crosses(1), 1, 0) + jnp.where(crosses(2), 1, 0))

    @pl.when(~is_line)
    def _():
        for device in ring_next:
            greet(device)
        pl.semaphore_wait(barrier, planes + 2)

    def remote(src, dst, send_sem, recv_sem, device):
        return pltpu.make_async_remote_copy(
            src_ref=src, dst_ref=dst, send_sem=send_sem, recv_sem=recv_sem, device_id=device, device_id_type=MESH)

    def s1_copy(a, turn):
        n = own_index(a, turn, g)
        return remote(xbuf.at[loan_index(a, turn, g)], cbuf.at[n], s1_send.at[a, turn - 1], c_recv.at[n],
                      chip(z, piece_of(p, turn), LINE))

    def lend_copy(a, turn):
        n = loan_index(a, turn, RING)
        return remote(xbuf.at[n], xbuf.at[n], x_send.at[a, RING, turn - 1], x_recv.at[a, turn - 1], chip(z, p, LINE))

    def cross_copy(a, turn, gg):
        n = toward + own_index(a, turn, gg)
        return remote(xbuf.at[loan_index(a, turn, gg)], cbuf.at[n], x_send.at[a, gg, turn - 1], c_recv.at[n],
                      chip(end_z, piece_of(p, turn), LINE))

    def line_copy(n, to, zz, sem):
        return remote(cbuf.at[n], cbuf.at[to], sem, c_recv.at[to], chip(zz, p, LINE))

    def pair_copy(n, sem):
        return remote(cbuf.at[n], cbuf.at[n], sem, c_recv.at[n], pair)

    def ring_copy(buf, n, to, way, sem):
        return remote(buf.at[n], rbuf.at[to], sem, r_recv.at[to], ring_next[way])

    def share_copy(n, sem):
        rows = rbuf.at[n, :, line_half]
        return remote(rows, rows, sem, r_recv.at[n], pair)

    def spot(dist, near):
        from_high = low_side == near
        inside = jnp.where(from_high, z + dist < lines, z >= dist)
        sd = jnp.where((dist == 0) | from_high, dist, dist + lines - 1)
        return sd, inside & (dist < lines)

    def drain(count, sem, buf):
        ref = buf.at[pl.ds(0, count)]
        pltpu.make_async_copy(ref, ref, sem).wait()

    def col_turn(sd, turn, dist, near):
        for a in range(2):
            for gg in (LINE, RING):
                n = group * sd + own_index(a, turn, gg)

                def one(n=n, gg=gg):
                    landed(cbuf.at[n], c_recv.at[n])
                    if near is None or near is False:
                        main_ok = True
                    else:
                        main_ok = ~at_end
                    if dist is None:
                        if turn in (1, 2):
                            main_ok = main_ok & ~crosses(turn)
                        line_copy(n, n + away, z - end_step, z_send.at[2 * lines - 1, turn]).start()
                        to, zz = n + toward, z + end_step
                    else:
                        to, zz = n + group, z + (end_step if near else -end_step)

                    def main():
                        line_copy(n, to, zz, z_send.at[sd, turn]).start()

                    if main_ok is True:
                        main()
                    else:
                        pl.when(main_ok)(main)
                    if not (dist is None and turn == 0 and gg == RING):
                        pair_copy(n, d_send.at[sd, turn]).start()

                if not (dist is None and turn == 0 and gg == LINE):
                    one()

    def feed_turn(sd, turn, dist, near):
        for a in range(2):
            for gg in range(2):
                n = group * sd + own_index(a, turn, gg)
                if not (dist is None and turn == 0 and gg == RING):
                    landed(cbuf.at[n], c_recv.at[n])
                way = (turn + gg) % 2
                to = group * sd + own_index(a, next_turn(turn, way), gg)
                ring_copy(cbuf, n, to, way, z_send.at[sd, turn]).start()

    def row_turn(way, passes):
        def action(sd, turn, dist, near):
            here = local_turn(turn)
            gg = (turn + way) % 2
            n = group * sd + own_index(0, here, gg)
            to = group * sd + own_index(0, next_turn(here, way), gg)
            for a in range(2):
                m, to_m = n + own_index(a, 0, 0), to + own_index(a, 0, 0)
                landed(rbuf.at[m], r_recv.at[m])
                if passes:
                    ring_copy(rbuf, m, to_m, way, z_send.at[sd, turn]).start()
                share_copy(m, d_send.at[sd, turn]).start()

        return action

    def gather_waits(base, skip_own):
        @pl.when(~is_root)
        def _():
            @pl.when(is_line)
            def _():
                for j in range(2 * planes):
                    landed(rbuf.at[base + j, :, line_half], r_recv.at[base + j])

            @pl.when(~is_line)
            def _():
                for j in range(2 * planes):
                    if not (skip_own and j == RING):
                        landed(cbuf.at[base + j], c_recv.at[base + j])

    def product(a, base, count, rows):
        lhs = rows[pl.ds(base, count), :, my_half].reshape(count * tok, rh)
        rhs = cbuf[pl.ds(base, count)].reshape(count * tok, ct)
        outs[a][...] += lax.dot_general(lhs, rhs, (((0,), (0,)), ((), ())), preferred_element_type=jnp.float32)

    def multiply(sd, skip_own=False):
        for a in range(2):
            base = group * sd + own_index(a, 0, 0)
            gather_waits(base, skip_own)

            @pl.when(is_root)
            def _():
                product(a, base, 2 * planes, cbuf)

            @pl.when(~is_root)
            def _():
                product(a, base, 2 * planes, rbuf)

    for a in range(2):
        load_own(a).wait()

        @pl.when(is_line)
        def _():
            n = own_index(a, 0, LINE)

            @pl.when(~at_end)
            def _():
                line_copy(n, n + toward, z + end_step, z_send.at[0, 0]).start()
            line_copy(n, n + away, z - end_step, z_send.at[2 * lines - 1, 0]).start()
            pair_copy(n, d_send.at[0, 0]).start()

        @pl.when(~is_line)
        def _():
            pair_copy(own_index(a, 0, RING), x_send.at[a, LINE, 0]).start()

    for turn in range(1, planes):
        for a in range(2):
            load(a, turn).wait()
            s1_copy(a, turn).start()
    for turn in range(1, 3):
        @pl.when(~is_line & ~at_end & crosses(turn))
        def _():
            for a in range(2):
                lend_copy(a, turn).start()
    for out in outs:
        out[...] = jnp.zeros_like(out)

    def send_cross(a, turn):
        cross_copy(a, turn, LINE).start()
        landed(xbuf.at[loan_index(a, turn, RING)], x_recv.at[a, turn - 1])
        cross_copy(a, turn, RING).start()

    def turns(block, r, shift, action):
        first = r - shift

        @pl.when(block + first // planes == 0)
        def _():
            action(0, first % planes, None, True)

        def along(near, u0, keep):
            dist = block + u0 // planes
            turn = u0 % planes
            sd, inside = spot(dist, near)

            @pl.when(inside & (dist > 0) & keep(dist, turn))
            def _():
                action(sd, turn, dist, near)

        along(True, r - shift + AHEAD, lambda dist, turn: ~at_end | (dist != 1) if turn in (1, 2) else True)
        along(False, r - shift - FAR_LAG + AHEAD, lambda dist, turn: True)
        u_x = planes + 1 + r - shift - CROSS_WAIT
        if u_x % planes in (1, 2):
            late = place == u_x % planes
            along(True, u_x, lambda dist, turn: at_end & (dist == 1) & ~(late & is_col(action)))

    def is_col(action):
        return action is col_turn

    def block_steps(block, carry):
        for r in range(planes):
            @pl.when(is_line)
            def _():
                if r == CROSS_AT % planes:
                    @pl.when((block == CROSS_AT // planes) & ~at_end)
                    def _():
                        for turn in range(1, 3):
                            @pl.when(place == turn)
                            def _():
                                for a in range(2):
                                    send_cross(a, turn)
                if r == CROSS_LATE % planes:
                    @pl.when((block == CROSS_LATE // planes) & ~at_end & (place == 0))
                    def _():
                        for a in range(2):
                            for turn in range(1, 3):
                                send_cross(a, turn)
                turns(block, r, 0, col_turn)

            @pl.when(~is_line & is_root)
            def _():
                turns(block, r, 0, feed_turn)

            @pl.when(~is_line & ~is_root)
            def _():
                @pl.when(fwd < planes - 1)
                def _():
                    turns(block, r, 0, row_turn(0, True))

                @pl.when(bwd < planes - 1)
                def _():
                    turns(block, r, 0, row_turn(1, True))

                @pl.when(fwd == planes - 1)
                def _():
                    turns(block, r, SPAN_LAG, row_turn(0, False))

                @pl.when(bwd == planes - 1)
                def _():
                    turns(block, r, SPAN_LAG, row_turn(1, False))

            at = r - MUL_LAG
            if (at - (planes - 1)) % planes == 0:
                @pl.when(block == (planes - 1 - at) // planes)
                def _():
                    multiply(0, True)
            for near, shift in ((True, 0), (False, FAR_LAG)):
                u0 = at - shift + AHEAD
                if u0 % planes == planes - 1:
                    dist = block + u0 // planes
                    sd, inside = spot(dist, near)

                    @pl.when(inside & (dist > 0) & ~(at_end & (dist == 1)))
                    def _():
                        multiply(sd)
            u0 = planes + 1 + at - CROSS_WAIT
            if u0 % planes == 2:
                @pl.when(at_end & ~slot_late & (block + u0 // planes == 1))
                def _():
                    multiply(toward // group)
        return carry

    steps = planes * lines - AHEAD + FAR_LAG + MUL_LAG
    lax.fori_loop(0, (steps + planes - 1) // planes, block_steps, 0)

    @pl.when(slot_late)
    def _():
        for a in range(2):
            @pl.when(is_line)
            def _():
                for gg in (LINE, RING):
                    n = toward + own_index(a, place, gg)
                    landed(cbuf.at[n], c_recv.at[n])
                    pair_copy(n, d_send.at[toward // group, place]).start()
        for a in range(2):
            gather_waits(toward + own_index(a, 0, 0), False)
            product(a, toward + own_index(a, 0, 0), 2 * planes, rbuf)

    def done(j, carry):
        dist = j % lines
        near = j < lines
        sd, inside = spot(dist, near)

        @pl.when(inside & (near | (dist > 0)))
        def _():
            for turn in range(planes):
                @pl.when(is_line)
                def _():
                    @pl.when(jnp.logical_not(near) | (~at_end & ~((dist == 0) & crosses(turn))))
                    def _():
                        drain(4, z_send.at[sd, turn], cbuf)

                    @pl.when(dist == 0)
                    def _():
                        drain(4, z_send.at[2 * lines - 1, turn], cbuf)
                    if turn == 0:
                        @pl.when(dist == 0)
                        def _():
                            drain(2, d_send.at[sd, turn], cbuf)

                        @pl.when(dist > 0)
                        def _():
                            drain(4, d_send.at[sd, turn], cbuf)
                    else:
                        drain(4, d_send.at[sd, turn], cbuf)

                @pl.when(~is_line)
                def _():
                    @pl.when(is_root | (fwd == 2))
                    def _():
                        drain(4, z_send.at[sd, turn], cbuf)

                    @pl.when(~is_root & (fwd != 2))
                    def _():
                        drain(2, z_send.at[sd, turn], cbuf)

                    @pl.when(~is_root)
                    def _():
                        rows = rbuf.at[pl.ds(0, 4), :, line_half]
                        pltpu.make_async_copy(rows, rows, d_send.at[sd, turn]).wait()
        return carry

    lax.fori_loop(0, 2 * lines, done, 0)
    for turn in range(1, planes):
        for a in range(2):
            s1_copy(a, turn).wait_send()
    for a in range(2):
        @pl.when(~is_line)
        def _():
            pair_copy(own_index(a, 0, RING), x_send.at[a, LINE, 0]).wait_send()
        for turn in range(1, 3):
            @pl.when(is_line & ~at_end & crosses(turn))
            def _():
                for gg in range(2):
                    cross_copy(a, turn, gg).wait_send()

            @pl.when(~is_line & ~at_end & crosses(turn))
            def _():
                lend_copy(a, turn).wait_send()


def fused(attn_input, mlp_input):
    groups, tiles = lax.axis_size("grp"), lax.axis_size("tile")
    tok, width = attn_input.shape
    ct, rh = width // ROWB, width // ROWB // groups
    norm_factor = 2.0 / (tok * tiles * groups)
    dma = pltpu.SemaphoreType.DMA
    group = 4 * ROWB
    total = group * (2 * ROWB - 1)
    hess = pl.pallas_call(
        kernel,
        out_shape=[jax.ShapeDtypeStruct((rh, ct), jnp.float32)] * 2,
        in_specs=[pl.BlockSpec(memory_space=IN_SPACE)] * 2,
        out_specs=[pl.BlockSpec(memory_space=pltpu.VMEM)] * 2,
        scratch_shapes=[
            pltpu.VMEM((4 * (ROWB - 1), tok, ct), jnp.bfloat16),
            pltpu.VMEM((total, tok, ct), jnp.bfloat16),
            pltpu.VMEM((total, tok, ct), jnp.bfloat16),
            dma((2,)), dma((2, ROWB - 1)), dma((2, 2)), dma((total,)), dma((total,)),
            dma((2, ROWB - 1)), dma((2, groups, 2)), dma((2 * ROWB - 1, ROWB)), dma((2 * ROWB, ROWB)),
        ],
        compiler_params=pltpu.CompilerParams(collective_id=0, has_side_effects=True, vmem_limit_bytes=VMEM_LIMIT),
    )(pltpu.with_memory_space_constraint(attn_input, pltpu.HBM), pltpu.with_memory_space_constraint(mlp_input, pltpu.HBM))
    return hess[0][None] * norm_factor, hess[1][None] * norm_factor


def body(attn_input, mlp_input):
    if lax.axis_size("grp") == 2 and lax.axis_size("tile") == ROWB * ROWB:
        return fused(attn_input, mlp_input)
    return (hessian_share(attn_input), hessian_share(mlp_input))


def solution(mesh):
    in_specs = (P(("grp", "tile"), None), P(("grp", "tile"), None))
    out_specs = (P("tile", "grp", None), P("tile", "grp", None))
    return jax.shard_map(body, mesh=mesh, in_specs=in_specs, out_specs=out_specs, check_vma=False)
```

```python
import jax
import jax.numpy as jnp
from jax import lax
from jax.experimental import pallas as pl
from jax.experimental.pallas import tpu as pltpu
from jax.sharding import PartitionSpec as P

ROWB = 4
TOKB = 32
MESH = pl.DeviceIdType.MESH
LINE = 0
RING = 1
AHEAD = 3
CROSS_AT = 3
CROSS_LATE = 9
CROSS_WAIT = 7
FAR_LAG = 1
SPAN_LAG = 3
MUL_LAG = 5
LATE_AT = 16
VMEM_LIMIT = 48 * 1024 * 1024
IN_SPACE = pltpu.HBM


def tile_first(inputs, tile_count):
    tok_rows, feat_width = inputs.shape
    col_blocks = tile_count // ROWB
    row_width = feat_width // ROWB
    col_width = feat_width // col_blocks

    def accumulate(turn_idx, partial_value):
        tok_block = lax.dynamic_slice_in_dim(inputs, turn_idx * TOKB, TOKB, 0)
        row_parts = tok_block.reshape(TOKB, ROWB, row_width).transpose(1, 0, 2)
        row_send = jnp.repeat(row_parts, col_blocks, axis=0)
        col_parts = tok_block.reshape(TOKB, col_blocks, col_width).transpose(1, 0, 2)
        col_send = jnp.tile(col_parts, (ROWB, 1, 1))
        rows_in, cols_in = (
            lax.all_to_all(row_send, "tile", split_axis=0, concat_axis=0, tiled=True),
            lax.all_to_all(col_send, "tile", split_axis=0, concat_axis=0, tiled=True),
        )
        rows_flat = rows_in.reshape(tile_count * TOKB, row_width)
        cols_flat = cols_in.reshape(tile_count * TOKB, col_width)
        return partial_value + lax.dot_general(
            rows_flat, cols_flat, (((0,), (0,)), ((), ())), preferred_element_type=jnp.float32
        )

    partial_value = lax.fori_loop(
        0, tok_rows // TOKB, accumulate, jnp.zeros((row_width, col_width), jnp.float32)
    )
    shares = lax.psum_scatter(partial_value, "grp", scatter_dimension=0, tiled=True)
    return shares[None]


def hessian_share(inputs):
    tile_count = lax.axis_size("tile")
    group_count = lax.axis_size("grp")
    norm_factor = 2.0 / (inputs.shape[0] * tile_count * group_count)
    shares = tile_first(inputs, tile_count)
    return shares * norm_factor


def ring_place(member):
    return member + (member // 2) * (1 - 2 * (member % 2))


def piece_of(home, turn):
    near = home + 1 - 2 * (home % 2)
    far = (home + 2) % ROWB
    return jnp.where(turn == 0, home, jnp.where(turn == 1, near, jnp.where(turn == 2, far, ROWB - 1 - home)))


def kernel(xa, xm, out_a, out_m, xbuf, cbuf, rbuf, own_sem, ld_sem, x_recv, c_recv, r_recv, s1_send, x_send, d_send, z_send):
    lines = planes = ROWB
    group = 4 * planes
    side = group * (lines - 1)
    total = group * (2 * lines - 1)
    g = lax.axis_index("grp")
    t = lax.axis_index("tile")
    z, p = t // planes, t % planes
    tok, _ = xa.shape
    ct = cbuf.shape[-1]
    rh = ct // 2
    xs = (xa, xm)
    outs = (out_a, out_m)
    is_line = g == LINE
    line_half = pl.ds(LINE * rh, rh)
    my_half = pl.ds(pl.multiple_of(g * rh, rh), rh)

    fwd = (ring_place(p) - ring_place(z) + planes) % planes
    bwd = (planes - fwd) % planes
    is_root = fwd == 0
    ring_fwd = ring_place((ring_place(p) + 1) % planes)
    ring_bwd = ring_place((ring_place(p) + planes - 1) % planes)
    fwd_is_near = ring_fwd == piece_of(p, 1)

    low_side = z < lines // 2
    upper = z // (lines // 2)
    end_z = upper * (lines - 1)
    at_end = z == end_z
    place = p + upper * (planes - 1 - 2 * p)
    beside = 1 + upper * (lines - 3)
    across = end_z + beside - z
    end_step = 2 * upper - 1
    toward = jnp.where(low_side, group, group + side)
    away = group + group + side - toward

    def crosses(turn):
        return (turn >= 1) & (turn <= 2) & ((place == 0) | (place == turn))

    def comes_late(turn, dist):
        return at_end & (dist == 1) & (turn >= 1) & (turn <= 2) & (place == turn)

    slot_late = at_end & ((place == 1) | (place == 2))

    def near_of(turn):
        return turn + 1 - 2 * (turn % 2)

    def far_of(turn):
        return (turn + 2) % planes

    def local_turn(turn):
        return jnp.where(
            is_root, turn, jnp.where(
                z == piece_of(p, 1), near_of(turn), jnp.where(z == piece_of(p, 2), far_of(turn), planes - 1 - turn)))

    def next_turn(turn, way):
        return jnp.where(fwd_is_near == (way == 0), near_of(turn), far_of(turn))

    def chip(zz, pp, gg):
        return (gg, zz * planes + pp)

    pair = chip(z, p, 1 - g)
    ring_next = [chip(z, ring_fwd, RING), chip(z, ring_bwd, RING)]

    def landed(ref, sem):
        pltpu.make_async_copy(ref, ref, sem).wait()

    def cols(block):
        return pl.ds(pl.multiple_of(block * ct, ct), ct)

    def own_index(a, turn, gg):
        return 2 * planes * a + 2 * turn + gg

    def loan_index(a, turn, gg):
        return (2 * gg + a) * (planes - 1) + turn - 1

    def load_own(a):
        return pltpu.make_async_copy(xs[a].at[:, cols(p)], cbuf.at[own_index(a, 0, g)], own_sem.at[a])

    def load(a, turn):
        return pltpu.make_async_copy(
            xs[a].at[:, cols(piece_of(p, turn))], xbuf.at[loan_index(a, turn, g)], ld_sem.at[a, turn - 1])

    for a in range(2):
        load_own(a).start()
    for turn in range(1, planes):
        for a in range(2):
            load(a, turn).start()

    barrier = pltpu.get_barrier_semaphore()

    def greet(device):
        pl.semaphore_signal(barrier, inc=1, device_id=device, device_id_type=MESH)

    greet(pair)

    @pl.when(is_line)
    def _():
        for turn in range(1, planes):
            for gg in range(2):
                greet(chip(z, piece_of(p, turn), gg))
        for turn in range(1, 3):
            @pl.when(crosses(turn))
            def _():
                greet(chip(across, piece_of(p, turn), LINE))

        @pl.when(z > 0)
        def _():
            greet(chip(z - 1, p, LINE))

        @pl.when(z < lines - 1)
        def _():
            greet(chip(z + 1, p, LINE))

        pl.semaphore_wait(
            barrier, planes + jnp.where(z > 0, 1, 0) + jnp.where(z < lines - 1, 1, 0)
            + jnp.where(crosses(1), 1, 0) + jnp.where(crosses(2), 1, 0))

    @pl.when(~is_line)
    def _():
        for device in ring_next:
            greet(device)
        pl.semaphore_wait(barrier, planes + 2)

    def remote(src, dst, send_sem, recv_sem, device):
        return pltpu.make_async_remote_copy(
            src_ref=src, dst_ref=dst, send_sem=send_sem, recv_sem=recv_sem, device_id=device, device_id_type=MESH)

    def s1_copy(a, turn):
        n = own_index(a, turn, g)
        return remote(xbuf.at[loan_index(a, turn, g)], cbuf.at[n], s1_send.at[a, turn - 1], c_recv.at[n],
                      chip(z, piece_of(p, turn), LINE))

    def lend_copy(a, turn):
        n = loan_index(a, turn, RING)
        return remote(xbuf.at[n], xbuf.at[n], x_send.at[a, RING, turn - 1], x_recv.at[a, turn - 1], chip(z, p, LINE))

    def cross_copy(a, turn, gg):
        n = toward + own_index(a, turn, gg)
        return remote(xbuf.at[loan_index(a, turn, gg)], cbuf.at[n], x_send.at[a, gg, turn - 1], c_recv.at[n],
                      chip(end_z, piece_of(p, turn), LINE))

    def line_copy(n, to, zz, sem):
        return remote(cbuf.at[n], cbuf.at[to], sem, c_recv.at[to], chip(zz, p, LINE))

    def pair_copy(n, sem):
        return remote(cbuf.at[n], cbuf.at[n], sem, c_recv.at[n], pair)

    def ring_copy(buf, n, to, way, sem):
        return remote(buf.at[n], rbuf.at[to], sem, r_recv.at[to], ring_next[way])

    def share_copy(n, sem):
        rows = rbuf.at[n, :, line_half]
        return remote(rows, rows, sem, r_recv.at[n], pair)

    def spot(dist, near):
        from_high = low_side == near
        inside = jnp.where(from_high, z + dist < lines, z >= dist)
        sd = jnp.where((dist == 0) | from_high, dist, dist + lines - 1)
        return sd, inside & (dist < lines)

    def drain(count, sem, buf):
        ref = buf.at[pl.ds(0, count)]
        pltpu.make_async_copy(ref, ref, sem).wait()

    def col_turn(sd, turn, dist, near):
        for a in range(2):
            for gg in (LINE, RING):
                n = group * sd + own_index(a, turn, gg)

                def one(n=n, gg=gg):
                    landed(cbuf.at[n], c_recv.at[n])
                    if near is None or near is False:
                        main_ok = True
                    else:
                        main_ok = ~at_end
                    if dist is None:
                        if turn in (1, 2):
                            main_ok = main_ok & ~crosses(turn)
                        line_copy(n, n + away, z - end_step, z_send.at[2 * lines - 1, turn]).start()
                        to, zz = n + toward, z + end_step
                    else:
                        to, zz = n + group, z + (end_step if near else -end_step)

                    def main():
                        line_copy(n, to, zz, z_send.at[sd, turn]).start()

                    if main_ok is True:
                        main()
                    else:
                        pl.when(main_ok)(main)
                    if not (dist is None and turn == 0 and gg == RING):
                        pair_copy(n, d_send.at[sd, turn]).start()

                if not (dist is None and turn == 0 and gg == LINE):
                    one()

    def feed_turn(sd, turn, dist, near):
        for a in range(2):
            for gg in range(2):
                n = group * sd + own_index(a, turn, gg)
                if not (dist is None and turn == 0 and gg == RING):
                    landed(cbuf.at[n], c_recv.at[n])
                way = (turn + gg) % 2
                to = group * sd + own_index(a, next_turn(turn, way), gg)
                ring_copy(cbuf, n, to, way, z_send.at[sd, turn]).start()

    def row_turn(way, passes):
        def action(sd, turn, dist, near):
            here = local_turn(turn)
            gg = (turn + way) % 2
            n = group * sd + own_index(0, here, gg)
            to = group * sd + own_index(0, next_turn(here, way), gg)
            for a in range(2):
                m, to_m = n + own_index(a, 0, 0), to + own_index(a, 0, 0)
                landed(rbuf.at[m], r_recv.at[m])
                if passes:
                    ring_copy(rbuf, m, to_m, way, z_send.at[sd, turn]).start()
                share_copy(m, d_send.at[sd, turn]).start()

        return action

    def gather_waits(base, skip_own):
        @pl.when(~is_root)
        def _():
            @pl.when(is_line)
            def _():
                for j in range(2 * planes):
                    landed(rbuf.at[base + j, :, line_half], r_recv.at[base + j])

            @pl.when(~is_line)
            def _():
                for j in range(2 * planes):
                    if not (skip_own and j == RING):
                        landed(cbuf.at[base + j], c_recv.at[base + j])

    def product(a, base, count, rows):
        lhs = rows[pl.ds(base, count), :, my_half].reshape(count * tok, rh)
        rhs = cbuf[pl.ds(base, count)].reshape(count * tok, ct)
        outs[a][...] += lax.dot_general(lhs, rhs, (((0,), (0,)), ((), ())), preferred_element_type=jnp.float32)

    def multiply(sd, skip_own=False):
        for a in range(2):
            base = group * sd + own_index(a, 0, 0)
            gather_waits(base, skip_own)

            @pl.when(is_root)
            def _():
                product(a, base, 2 * planes, cbuf)

            @pl.when(~is_root)
            def _():
                product(a, base, 2 * planes, rbuf)

    for a in range(2):
        load_own(a).wait()

        @pl.when(is_line)
        def _():
            n = own_index(a, 0, LINE)

            @pl.when(~at_end)
            def _():
                line_copy(n, n + toward, z + end_step, z_send.at[0, 0]).start()
            line_copy(n, n + away, z - end_step, z_send.at[2 * lines - 1, 0]).start()
            pair_copy(n, d_send.at[0, 0]).start()

        @pl.when(~is_line)
        def _():
            pair_copy(own_index(a, 0, RING), x_send.at[a, LINE, 0]).start()

    for turn in range(1, planes):
        for a in range(2):
            load(a, turn).wait()
            s1_copy(a, turn).start()
    for turn in range(1, 3):
        @pl.when(~is_line & ~at_end & crosses(turn))
        def _():
            for a in range(2):
                lend_copy(a, turn).start()
    for out in outs:
        out[...] = jnp.zeros_like(out)

    def send_cross(a, turn):
        cross_copy(a, turn, LINE).start()
        landed(xbuf.at[loan_index(a, turn, RING)], x_recv.at[a, turn - 1])
        cross_copy(a, turn, RING).start()

    def turns(block, r, shift, action):
        first = r - shift

        @pl.when(block + first // planes == 0)
        def _():
            action(0, first % planes, None, True)

        def along(near, u0, keep):
            dist = block + u0 // planes
            turn = u0 % planes
            sd, inside = spot(dist, near)

            @pl.when(inside & (dist > 0) & keep(dist, turn))
            def _():
                action(sd, turn, dist, near)

        along(True, r - shift + AHEAD, lambda dist, turn: ~at_end | (dist != 1) if turn in (1, 2) else True)
        along(False, r - shift - FAR_LAG + AHEAD, lambda dist, turn: True)
        u_x = planes + 1 + r - shift - CROSS_WAIT
        if u_x % planes in (1, 2):
            late = place == u_x % planes
            along(True, u_x, lambda dist, turn: at_end & (dist == 1) & ~(late & is_col(action)))

    def is_col(action):
        return action is col_turn

    def block_steps(block, carry):
        for r in range(planes):
            @pl.when(is_line)
            def _():
                if r == CROSS_AT % planes:
                    @pl.when((block == CROSS_AT // planes) & ~at_end)
                    def _():
                        for turn in range(1, 3):
                            @pl.when(place == turn)
                            def _():
                                for a in range(2):
                                    send_cross(a, turn)
                if r == CROSS_LATE % planes:
                    @pl.when((block == CROSS_LATE // planes) & ~at_end & (place == 0))
                    def _():
                        for a in range(2):
                            for turn in range(1, 3):
                                send_cross(a, turn)
                turns(block, r, 0, col_turn)

            @pl.when(~is_line & is_root)
            def _():
                turns(block, r, 0, feed_turn)

            @pl.when(~is_line & ~is_root)
            def _():
                @pl.when(fwd < planes - 1)
                def _():
                    turns(block, r, 0, row_turn(0, True))

                @pl.when(bwd < planes - 1)
                def _():
                    turns(block, r, 0, row_turn(1, True))

                @pl.when(fwd == planes - 1)
                def _():
                    turns(block, r, SPAN_LAG, row_turn(0, False))

                @pl.when(bwd == planes - 1)
                def _():
                    turns(block, r, SPAN_LAG, row_turn(1, False))

            if r == LATE_AT % planes:
                @pl.when(slot_late & is_line & (block == LATE_AT // planes))
                def _():
                    for a in range(2):
                        for gg in (LINE, RING):
                            n = toward + own_index(a, place, gg)
                            landed(cbuf.at[n], c_recv.at[n])
                            pair_copy(n, d_send.at[toward // group, place]).start()

            at = r - MUL_LAG
            if (at - (planes - 1)) % planes == 0:
                @pl.when(block == (planes - 1 - at) // planes)
                def _():
                    multiply(0, True)
            for near, shift in ((True, 0), (False, FAR_LAG)):
                u0 = at - shift + AHEAD
                if u0 % planes == planes - 1:
                    dist = block + u0 // planes
                    sd, inside = spot(dist, near)

                    @pl.when(inside & (dist > 0) & ~(at_end & (dist == 1)))
                    def _():
                        multiply(sd)
            u0 = planes + 1 + at - CROSS_WAIT
            if u0 % planes == 2:
                @pl.when(at_end & ~slot_late & (block + u0 // planes == 1))
                def _():
                    multiply(toward // group)
        return carry

    steps = planes * lines - AHEAD + FAR_LAG + MUL_LAG
    lax.fori_loop(0, (steps + planes - 1) // planes, block_steps, 0)

    @pl.when(slot_late)
    def _():
        for a in range(2):
            gather_waits(toward + own_index(a, 0, 0), False)
            product(a, toward + own_index(a, 0, 0), 2 * planes, rbuf)

    def done(j, carry):
        dist = j % lines
        near = j < lines
        sd, inside = spot(dist, near)

        @pl.when(inside & (near | (dist > 0)))
        def _():
            for turn in range(planes):
                @pl.when(is_line)
                def _():
                    @pl.when(jnp.logical_not(near) | (~at_end & ~((dist == 0) & crosses(turn))))
                    def _():
                        drain(4, z_send.at[sd, turn], cbuf)

                    @pl.when(dist == 0)
                    def _():
                        drain(4, z_send.at[2 * lines - 1, turn], cbuf)
                    if turn == 0:
                        @pl.when(dist == 0)
                        def _():
                            drain(2, d_send.at[sd, turn], cbuf)

                        @pl.when(dist > 0)
                        def _():
                            drain(4, d_send.at[sd, turn], cbuf)
                    else:
                        drain(4, d_send.at[sd, turn], cbuf)

                @pl.when(~is_line)
                def _():
                    @pl.when(is_root | (fwd == 2))
                    def _():
                        drain(4, z_send.at[sd, turn], cbuf)

                    @pl.when(~is_root & (fwd != 2))
                    def _():
                        drain(2, z_send.at[sd, turn], cbuf)

                    @pl.when(~is_root)
                    def _():
                        rows = rbuf.at[pl.ds(0, 4), :, line_half]
                        pltpu.make_async_copy(rows, rows, d_send.at[sd, turn]).wait()
        return carry

    lax.fori_loop(0, 2 * lines, done, 0)
    for turn in range(1, planes):
        for a in range(2):
            s1_copy(a, turn).wait_send()
    for a in range(2):
        @pl.when(~is_line)
        def _():
            pair_copy(own_index(a, 0, RING), x_send.at[a, LINE, 0]).wait_send()
        for turn in range(1, 3):
            @pl.when(is_line & ~at_end & crosses(turn))
            def _():
                for gg in range(2):
                    cross_copy(a, turn, gg).wait_send()

            @pl.when(~is_line & ~at_end & crosses(turn))
            def _():
                lend_copy(a, turn).wait_send()


def fused(attn_input, mlp_input):
    groups, tiles = lax.axis_size("grp"), lax.axis_size("tile")
    tok, width = attn_input.shape
    ct, rh = width // ROWB, width // ROWB // groups
    norm_factor = 2.0 / (tok * tiles * groups)
    dma = pltpu.SemaphoreType.DMA
    group = 4 * ROWB
    total = group * (2 * ROWB - 1)
    hess = pl.pallas_call(
        kernel,
        out_shape=[jax.ShapeDtypeStruct((rh, ct), jnp.float32)] * 2,
        in_specs=[pl.BlockSpec(memory_space=IN_SPACE)] * 2,
        out_specs=[pl.BlockSpec(memory_space=pltpu.VMEM)] * 2,
        scratch_shapes=[
            pltpu.VMEM((4 * (ROWB - 1), tok, ct), jnp.bfloat16),
            pltpu.VMEM((total, tok, ct), jnp.bfloat16),
            pltpu.VMEM((total, tok, ct), jnp.bfloat16),
            dma((2,)), dma((2, ROWB - 1)), dma((2, 2)), dma((total,)), dma((total,)),
            dma((2, ROWB - 1)), dma((2, groups, 2)), dma((2 * ROWB - 1, ROWB)), dma((2 * ROWB, ROWB)),
        ],
        compiler_params=pltpu.CompilerParams(collective_id=0, has_side_effects=True, vmem_limit_bytes=VMEM_LIMIT),
    )(pltpu.with_memory_space_constraint(attn_input, pltpu.HBM), pltpu.with_memory_space_constraint(mlp_input, pltpu.HBM))
    return hess[0][None] * norm_factor, hess[1][None] * norm_factor


def body(attn_input, mlp_input):
    if lax.axis_size("grp") == 2 and lax.axis_size("tile") == ROWB * ROWB:
        return fused(attn_input, mlp_input)
    return (hessian_share(attn_input), hessian_share(mlp_input))


def solution(mesh):
    in_specs = (P(("grp", "tile"), None), P(("grp", "tile"), None))
    out_specs = (P("tile", "grp", None), P("tile", "grp", None))
    return jax.shard_map(body, mesh=mesh, in_specs=in_specs, out_specs=out_specs, check_vma=False)
```

```python
import jax
import jax.numpy as jnp
from jax import lax
from jax.experimental import pallas as pl
from jax.experimental.pallas import tpu as pltpu
from jax.sharding import PartitionSpec as P

ROWB = 4
TOKB = 32
MESH = pl.DeviceIdType.MESH
LINE = 0
RING = 1
AHEAD = 3
CROSS_AT = 3
CROSS_LATE = 9
CROSS_WAIT = 7
FAR_LAG = 1
SPAN_LAG = 3
MUL_LAG = 5
LATE_AT = 16
VMEM_LIMIT = 48 * 1024 * 1024
IN_SPACE = pltpu.HBM


def tile_first(inputs, tile_count):
    tok_rows, feat_width = inputs.shape
    col_blocks = tile_count // ROWB
    row_width = feat_width // ROWB
    col_width = feat_width // col_blocks

    def accumulate(turn_idx, partial_value):
        tok_block = lax.dynamic_slice_in_dim(inputs, turn_idx * TOKB, TOKB, 0)
        row_parts = tok_block.reshape(TOKB, ROWB, row_width).transpose(1, 0, 2)
        row_send = jnp.repeat(row_parts, col_blocks, axis=0)
        col_parts = tok_block.reshape(TOKB, col_blocks, col_width).transpose(1, 0, 2)
        col_send = jnp.tile(col_parts, (ROWB, 1, 1))
        rows_in, cols_in = (
            lax.all_to_all(row_send, "tile", split_axis=0, concat_axis=0, tiled=True),
            lax.all_to_all(col_send, "tile", split_axis=0, concat_axis=0, tiled=True),
        )
        rows_flat = rows_in.reshape(tile_count * TOKB, row_width)
        cols_flat = cols_in.reshape(tile_count * TOKB, col_width)
        return partial_value + lax.dot_general(
            rows_flat, cols_flat, (((0,), (0,)), ((), ())), preferred_element_type=jnp.float32
        )

    partial_value = lax.fori_loop(
        0, tok_rows // TOKB, accumulate, jnp.zeros((row_width, col_width), jnp.float32)
    )
    shares = lax.psum_scatter(partial_value, "grp", scatter_dimension=0, tiled=True)
    return shares[None]


def hessian_share(inputs):
    tile_count = lax.axis_size("tile")
    group_count = lax.axis_size("grp")
    norm_factor = 2.0 / (inputs.shape[0] * tile_count * group_count)
    shares = tile_first(inputs, tile_count)
    return shares * norm_factor


def ring_place(member):
    return member + (member // 2) * (1 - 2 * (member % 2))


def piece_of(home, turn):
    near = home + 1 - 2 * (home % 2)
    far = (home + 2) % ROWB
    return jnp.where(turn == 0, home, jnp.where(turn == 1, near, jnp.where(turn == 2, far, ROWB - 1 - home)))


def kernel(xa, xm, out, xbuf, buf, own_sem, ld_sem, x_recv, c_recv, r_recv, s1_send, x_send, d_send, z_send, f_send):
    lines = planes = ROWB
    group = 4 * planes
    side = group * (lines - 1)
    total = group * (2 * lines - 1)
    g = lax.axis_index("grp")
    t = lax.axis_index("tile")
    z, p = t // planes, t % planes
    tok, _ = xa.shape
    ct = buf.shape[-1]
    cbuf, rbuf = buf.at[pl.ds(0, total)], buf.at[pl.ds(total, total)]
    rh = ct // 2
    xs = (xa, xm)
    is_line = g == LINE
    line_half = pl.ds(LINE * rh, rh)
    my_half = pl.ds(pl.multiple_of(g * rh, rh), rh)

    fwd = (ring_place(p) - ring_place(z) + planes) % planes
    bwd = (planes - fwd) % planes
    is_root = fwd == 0
    ring_fwd = ring_place((ring_place(p) + 1) % planes)
    ring_bwd = ring_place((ring_place(p) + planes - 1) % planes)
    fwd_is_near = ring_fwd == piece_of(p, 1)

    low_side = z < lines // 2
    upper = z // (lines // 2)
    end_z = upper * (lines - 1)
    at_end = z == end_z
    place = p + upper * (planes - 1 - 2 * p)
    beside = 1 + upper * (lines - 3)
    across = end_z + beside - z
    end_step = 2 * upper - 1
    toward = jnp.where(low_side, group, group + side)
    away = group + group + side - toward

    def crosses(turn):
        return (turn >= 1) & (turn <= 2) & ((place == 0) | (place == turn))

    def comes_late(turn, dist):
        return at_end & (dist == 1) & (turn >= 1) & (turn <= 2) & (place == turn)

    slot_late = at_end & ((place == 1) | (place == 2))

    def near_of(turn):
        return turn + 1 - 2 * (turn % 2)

    def far_of(turn):
        return (turn + 2) % planes

    def local_turn(turn):
        return jnp.where(
            is_root, turn, jnp.where(
                z == piece_of(p, 1), near_of(turn), jnp.where(z == piece_of(p, 2), far_of(turn), planes - 1 - turn)))

    def next_turn(turn, way):
        return jnp.where(fwd_is_near == (way == 0), near_of(turn), far_of(turn))

    def chip(zz, pp, gg):
        return (gg, zz * planes + pp)

    pair = chip(z, p, 1 - g)
    ring_next = [chip(z, ring_fwd, RING), chip(z, ring_bwd, RING)]

    def landed(ref, sem):
        pltpu.make_async_copy(ref, ref, sem).wait()

    def cols(block):
        return pl.ds(pl.multiple_of(block * ct, ct), ct)

    def own_index(a, turn, gg):
        return 2 * planes * a + 2 * turn + gg

    def loan_index(a, turn, gg):
        return (2 * gg + a) * (planes - 1) + turn - 1

    def load_own(a):
        return pltpu.make_async_copy(xs[a].at[:, cols(p)], cbuf.at[own_index(a, 0, g)], own_sem.at[a])

    def load(a, turn):
        return pltpu.make_async_copy(
            xs[a].at[:, cols(piece_of(p, turn))], xbuf.at[loan_index(a, turn, g)], ld_sem.at[a, turn - 1])

    for a in range(2):
        load_own(a).start()
    for turn in range(1, planes):
        for a in range(2):
            load(a, turn).start()

    barrier = pltpu.get_barrier_semaphore()

    def greet(device):
        pl.semaphore_signal(barrier, inc=1, device_id=device, device_id_type=MESH)

    greet(pair)

    @pl.when(is_line)
    def _():
        for turn in range(1, planes):
            for gg in range(2):
                greet(chip(z, piece_of(p, turn), gg))
        for turn in range(1, 3):
            @pl.when(crosses(turn))
            def _():
                greet(chip(across, piece_of(p, turn), LINE))

        @pl.when(z > 0)
        def _():
            greet(chip(z - 1, p, LINE))

        @pl.when(z < lines - 1)
        def _():
            greet(chip(z + 1, p, LINE))

        pl.semaphore_wait(
            barrier, planes + 2 + jnp.where(z > 0, 1, 0) + jnp.where(z < lines - 1, 1, 0)
            + jnp.where(crosses(1), 1, 0) + jnp.where(crosses(2), 1, 0))

    @pl.when(~is_line)
    def _():
        for device in ring_next:
            greet(device)
        for chip_next in (ring_fwd, ring_bwd):
            greet(chip(z, chip_next, LINE))
        pl.semaphore_wait(barrier, planes + 2)

    def remote(src, dst, send_sem, recv_sem, device):
        return pltpu.make_async_remote_copy(
            src_ref=src, dst_ref=dst, send_sem=send_sem, recv_sem=recv_sem, device_id=device, device_id_type=MESH)

    def s1_copy(a, turn):
        n = own_index(a, turn, g)
        return remote(xbuf.at[loan_index(a, turn, g)], cbuf.at[n], s1_send.at[a, turn - 1], c_recv.at[n],
                      chip(z, piece_of(p, turn), LINE))

    def lend_copy(a, turn):
        n = loan_index(a, turn, RING)
        return remote(xbuf.at[n], xbuf.at[n], x_send.at[a, RING, turn - 1], x_recv.at[a, turn - 1], chip(z, p, LINE))

    def cross_copy(a, turn, gg):
        n = toward + own_index(a, turn, gg)
        return remote(xbuf.at[loan_index(a, turn, gg)], cbuf.at[n], x_send.at[a, gg, turn - 1], c_recv.at[n],
                      chip(end_z, piece_of(p, turn), LINE))

    def line_copy(n, to, zz, sem):
        return remote(cbuf.at[n], cbuf.at[to], sem, c_recv.at[to], chip(zz, p, LINE))

    def pair_copy(n, sem):
        return remote(cbuf.at[n], cbuf.at[n], sem, c_recv.at[n], pair)

    def ring_copy(buf, n, to, way, sem):
        return remote(buf.at[n], rbuf.at[to], sem, r_recv.at[to], ring_next[way])

    def share_copy(n, sem):
        rows = rbuf.at[n, :, line_half]
        return remote(rows, rows, sem, r_recv.at[n], pair)

    def spot(dist, near):
        from_high = low_side == near
        inside = jnp.where(from_high, z + dist < lines, z >= dist)
        sd = jnp.where((dist == 0) | from_high, dist, dist + lines - 1)
        return sd, inside & (dist < lines)

    def drain(count, sem, buf):
        ref = buf.at[pl.ds(0, count)]
        pltpu.make_async_copy(ref, ref, sem).wait()

    def feed(sd, a, turn, gg):
        way = (turn + gg) % 2
        base = group * sd
        to = base + own_index(a, next_turn(turn, way), gg)

        @pl.when(is_root)
        def _():
            ring_copy(cbuf, base + own_index(a, turn, gg), to, way, f_send.at[sd, turn]).start()

    def col_turn(sd, turn, dist, near):
        for a in range(2):
            for gg in (LINE, RING):
                n = group * sd + own_index(a, turn, gg)

                def one(n=n, gg=gg):
                    landed(cbuf.at[n], c_recv.at[n])
                    if near is None or near is False:
                        main_ok = True
                    else:
                        main_ok = ~at_end
                    if dist is None:
                        if turn in (1, 2):
                            main_ok = main_ok & ~crosses(turn)
                        line_copy(n, n + away, z - end_step, z_send.at[2 * lines - 1, turn]).start()
                        to, zz = n + toward, z + end_step
                    else:
                        to, zz = n + group, z + (end_step if near else -end_step)

                    def main():
                        line_copy(n, to, zz, z_send.at[sd, turn]).start()

                    if main_ok is True:
                        main()
                    else:
                        pl.when(main_ok)(main)
                    feed(sd, a, turn, gg)
                    if not (dist is None and turn == 0 and gg == RING):
                        pair_copy(n, d_send.at[sd, turn]).start()

                if not (dist is None and turn == 0 and gg == LINE):
                    one()

    def row_turn(way, passes):
        def action(sd, turn, dist, near):
            here = local_turn(turn)
            gg = (turn + way) % 2
            n = group * sd + own_index(0, here, gg)
            to = group * sd + own_index(0, next_turn(here, way), gg)
            for a in range(2):
                m, to_m = n + own_index(a, 0, 0), to + own_index(a, 0, 0)
                landed(rbuf.at[m], r_recv.at[m])
                if passes:
                    ring_copy(rbuf, m, to_m, way, z_send.at[sd, turn]).start()
                share_copy(m, d_send.at[sd, turn]).start()

        return action

    def gather_waits(base, skip_own):
        @pl.when(is_line & ~is_root)
        def _():
            for j in range(2 * planes):
                landed(rbuf.at[base + j, :, line_half], r_recv.at[base + j])

        @pl.when(~is_line)
        def _():
            for j in range(2 * planes):
                if not (skip_own and j == RING):
                    landed(cbuf.at[base + j], c_recv.at[base + j])

    rows_from = jnp.where(is_root, 0, total)

    def multiply(sd, skip_own=False):
        def one(a, carry):
            base = group * sd + own_index(a, 0, 0)
            gather_waits(base, skip_own)
            lhs = buf[pl.ds(base + rows_from, 2 * planes), :, my_half].reshape(2 * planes * tok, rh)
            rhs = buf[pl.ds(base, 2 * planes)].reshape(2 * planes * tok, ct)
            out[a] += lax.dot_general(lhs, rhs, (((0,), (0,)), ((), ())), preferred_element_type=jnp.float32)
            return carry

        lax.fori_loop(0, 2, one, 0)

    for a in range(2):
        load_own(a).wait()

        @pl.when(is_line)
        def _():
            n = own_index(a, 0, LINE)

            @pl.when(~at_end)
            def _():
                line_copy(n, n + toward, z + end_step, z_send.at[0, 0]).start()
            line_copy(n, n + away, z - end_step, z_send.at[2 * lines - 1, 0]).start()
            feed(0, a, 0, LINE)
            pair_copy(n, d_send.at[0, 0]).start()

        @pl.when(~is_line)
        def _():
            pair_copy(own_index(a, 0, RING), x_send.at[a, LINE, 0]).start()

    for turn in range(1, planes):
        for a in range(2):
            load(a, turn).wait()
            s1_copy(a, turn).start()
    for turn in range(1, 3):
        @pl.when(~is_line & ~at_end & crosses(turn))
        def _():
            for a in range(2):
                lend_copy(a, turn).start()
    for a in range(2):
        out[a] = jnp.zeros_like(out[a])

    def send_cross(a, turn):
        cross_copy(a, turn, LINE).start()
        landed(xbuf.at[loan_index(a, turn, RING)], x_recv.at[a, turn - 1])
        cross_copy(a, turn, RING).start()

    def turns(block, r, shift, action):
        first = r - shift

        @pl.when(block + first // planes == 0)
        def _():
            action(0, first % planes, None, True)

        def along(near, u0, keep):
            dist = block + u0 // planes
            turn = u0 % planes
            sd, inside = spot(dist, near)

            @pl.when(inside & (dist > 0) & keep(dist, turn))
            def _():
                action(sd, turn, dist, near)

        along(True, r - shift + AHEAD, lambda dist, turn: ~at_end | (dist != 1) if turn in (1, 2) else True)
        along(False, r - shift - FAR_LAG + AHEAD, lambda dist, turn: True)
        u_x = planes + 1 + r - shift - CROSS_WAIT
        if u_x % planes in (1, 2):
            late = place == u_x % planes
            along(True, u_x, lambda dist, turn: at_end & (dist == 1) & ~(late & is_col(action)))

    def is_col(action):
        return action is col_turn

    def block_steps(block, carry):
        for r in range(planes):
            @pl.when(is_line)
            def _():
                if r == CROSS_AT % planes:
                    @pl.when((block == CROSS_AT // planes) & ~at_end)
                    def _():
                        for turn in range(1, 3):
                            @pl.when(place == turn)
                            def _():
                                for a in range(2):
                                    send_cross(a, turn)
                if r == CROSS_LATE % planes:
                    @pl.when((block == CROSS_LATE // planes) & ~at_end & (place == 0))
                    def _():
                        for a in range(2):
                            for turn in range(1, 3):
                                send_cross(a, turn)
                turns(block, r, 0, col_turn)

            @pl.when(~is_line & ~is_root)
            def _():
                @pl.when(fwd < planes - 1)
                def _():
                    turns(block, r, 0, row_turn(0, True))

                @pl.when(bwd < planes - 1)
                def _():
                    turns(block, r, 0, row_turn(1, True))

                @pl.when(fwd == planes - 1)
                def _():
                    turns(block, r, SPAN_LAG, row_turn(0, False))

                @pl.when(bwd == planes - 1)
                def _():
                    turns(block, r, SPAN_LAG, row_turn(1, False))

            if r == LATE_AT % planes:
                @pl.when(slot_late & is_line & (block == LATE_AT // planes))
                def _():
                    for a in range(2):
                        for gg in (LINE, RING):
                            n = toward + own_index(a, place, gg)
                            landed(cbuf.at[n], c_recv.at[n])
                            pair_copy(n, d_send.at[toward // group, place]).start()

            at = r - MUL_LAG
            if (at - (planes - 1)) % planes == 0:
                @pl.when(block == (planes - 1 - at) // planes)
                def _():
                    multiply(0, True)
            for near, shift in ((True, 0), (False, FAR_LAG)):
                u0 = at - shift + AHEAD
                if u0 % planes == planes - 1:
                    dist = block + u0 // planes
                    sd, inside = spot(dist, near)

                    @pl.when(inside & (dist > 0) & ~(at_end & (dist == 1)))
                    def _():
                        multiply(sd)
            u0 = planes + 1 + at - CROSS_WAIT
            if u0 % planes == 2:
                @pl.when(at_end & ~slot_late & (block + u0 // planes == 1))
                def _():
                    multiply(toward // group)
        return carry

    steps = planes * lines - AHEAD + FAR_LAG + MUL_LAG
    lax.fori_loop(0, (steps + planes - 1) // planes, block_steps, 0)

    def done(j, carry):
        dist = j % lines
        near = j < lines
        sd, inside = spot(dist, near)

        @pl.when(inside & (near | (dist > 0)))
        def _():
            for turn in range(planes):
                @pl.when(is_line)
                def _():
                    @pl.when(is_root)
                    def _():
                        drain(4, f_send.at[sd, turn], cbuf)

                    @pl.when(jnp.logical_not(near) | (~at_end & ~((dist == 0) & crosses(turn))))
                    def _():
                        drain(4, z_send.at[sd, turn], cbuf)

                    @pl.when(dist == 0)
                    def _():
                        drain(4, z_send.at[2 * lines - 1, turn], cbuf)
                    if turn == 0:
                        @pl.when(dist == 0)
                        def _():
                            drain(2, d_send.at[sd, turn], cbuf)

                        @pl.when(dist > 0)
                        def _():
                            drain(4, d_send.at[sd, turn], cbuf)
                    else:
                        drain(4, d_send.at[sd, turn], cbuf)

                @pl.when(~is_line)
                def _():
                    @pl.when(fwd == 2)
                    def _():
                        drain(4, z_send.at[sd, turn], cbuf)

                    @pl.when(~is_root & (fwd != 2))
                    def _():
                        drain(2, z_send.at[sd, turn], cbuf)

                    @pl.when(~is_root)
                    def _():
                        rows = rbuf.at[pl.ds(0, 4), :, line_half]
                        pltpu.make_async_copy(rows, rows, d_send.at[sd, turn]).wait()
        return carry

    lax.fori_loop(0, 2 * lines, done, 0)
    for turn in range(1, planes):
        for a in range(2):
            s1_copy(a, turn).wait_send()
    for a in range(2):
        @pl.when(~is_line)
        def _():
            pair_copy(own_index(a, 0, RING), x_send.at[a, LINE, 0]).wait_send()
        for turn in range(1, 3):
            @pl.when(is_line & ~at_end & crosses(turn))
            def _():
                for gg in range(2):
                    cross_copy(a, turn, gg).wait_send()

            @pl.when(~is_line & ~at_end & crosses(turn))
            def _():
                lend_copy(a, turn).wait_send()

    @pl.when(slot_late)
    def _():
        multiply(toward // group)


def fused(attn_input, mlp_input):
    groups, tiles = lax.axis_size("grp"), lax.axis_size("tile")
    tok, width = attn_input.shape
    ct, rh = width // ROWB, width // ROWB // groups
    norm_factor = 2.0 / (tok * tiles * groups)
    dma = pltpu.SemaphoreType.DMA
    group = 4 * ROWB
    total = group * (2 * ROWB - 1)
    hess = pl.pallas_call(
        kernel,
        out_shape=jax.ShapeDtypeStruct((2, rh, ct), jnp.float32),
        in_specs=[pl.BlockSpec(memory_space=IN_SPACE)] * 2,
        out_specs=pl.BlockSpec(memory_space=pltpu.VMEM),
        scratch_shapes=[
            pltpu.VMEM((4 * (ROWB - 1), tok, ct), jnp.bfloat16),
            pltpu.VMEM((2 * total, tok, ct), jnp.bfloat16),
            dma((2,)), dma((2, ROWB - 1)), dma((2, 2)), dma((total,)), dma((total,)),
            dma((2, ROWB - 1)), dma((2, groups, 2)), dma((2 * ROWB - 1, ROWB)), dma((2 * ROWB, ROWB)),
            dma((2 * ROWB - 1, ROWB)),
        ],
        compiler_params=pltpu.CompilerParams(collective_id=0, has_side_effects=True, vmem_limit_bytes=VMEM_LIMIT),
    )(pltpu.with_memory_space_constraint(attn_input, pltpu.HBM), pltpu.with_memory_space_constraint(mlp_input, pltpu.HBM))
    return hess[0][None] * norm_factor, hess[1][None] * norm_factor


def body(attn_input, mlp_input):
    if lax.axis_size("grp") == 2 and lax.axis_size("tile") == ROWB * ROWB:
        return fused(attn_input, mlp_input)
    return (hessian_share(attn_input), hessian_share(mlp_input))


def solution(mesh):
    in_specs = (P(("grp", "tile"), None), P(("grp", "tile"), None))
    out_specs = (P("tile", "grp", None), P("tile", "grp", None))
    return jax.shard_map(body, mesh=mesh, in_specs=in_specs, out_specs=out_specs, check_vma=False)
```

```python
import jax
import jax.numpy as jnp
from jax import lax
from jax.experimental import pallas as pl
from jax.experimental.pallas import tpu as pltpu
from jax.sharding import PartitionSpec as P

ROWB = 4
TOKB = 32
MESH = pl.DeviceIdType.MESH
LINE = 0
RING = 1
AHEAD = 3
CROSS_AT = 4
CROSS_LATE = 9
CROSS_WAIT = 8
FAR_LAG = 1
SPAN_LAG = 4
MUL_LAG = 6
LATE_AT = 17
VMEM_LIMIT = 48 * 1024 * 1024
IN_SPACE = pltpu.HBM


def tile_first(inputs, tile_count):
    tok_rows, feat_width = inputs.shape
    col_blocks = tile_count // ROWB
    row_width = feat_width // ROWB
    col_width = feat_width // col_blocks

    def accumulate(turn_idx, partial_value):
        tok_block = lax.dynamic_slice_in_dim(inputs, turn_idx * TOKB, TOKB, 0)
        row_parts = tok_block.reshape(TOKB, ROWB, row_width).transpose(1, 0, 2)
        row_send = jnp.repeat(row_parts, col_blocks, axis=0)
        col_parts = tok_block.reshape(TOKB, col_blocks, col_width).transpose(1, 0, 2)
        col_send = jnp.tile(col_parts, (ROWB, 1, 1))
        rows_in, cols_in = (
            lax.all_to_all(row_send, "tile", split_axis=0, concat_axis=0, tiled=True),
            lax.all_to_all(col_send, "tile", split_axis=0, concat_axis=0, tiled=True),
        )
        rows_flat = rows_in.reshape(tile_count * TOKB, row_width)
        cols_flat = cols_in.reshape(tile_count * TOKB, col_width)
        return partial_value + lax.dot_general(
            rows_flat, cols_flat, (((0,), (0,)), ((), ())), preferred_element_type=jnp.float32
        )

    partial_value = lax.fori_loop(
        0, tok_rows // TOKB, accumulate, jnp.zeros((row_width, col_width), jnp.float32)
    )
    shares = lax.psum_scatter(partial_value, "grp", scatter_dimension=0, tiled=True)
    return shares[None]


def hessian_share(inputs):
    tile_count = lax.axis_size("tile")
    group_count = lax.axis_size("grp")
    norm_factor = 2.0 / (inputs.shape[0] * tile_count * group_count)
    shares = tile_first(inputs, tile_count)
    return shares * norm_factor


def ring_place(member):
    return member + (member // 2) * (1 - 2 * (member % 2))


def piece_of(home, turn):
    near = home + 1 - 2 * (home % 2)
    far = (home + 2) % ROWB
    return jnp.where(turn == 0, home, jnp.where(turn == 1, near, jnp.where(turn == 2, far, ROWB - 1 - home)))


def kernel(xa, xm, out, xbuf, buf, own_sem, ld_sem, x_recv, c_recv, r_recv, s1_send, x_send, d_send, z_send, f_send):
    lines = planes = ROWB
    group = 4 * planes
    side = group * (lines - 1)
    total = group * (2 * lines - 1)
    g = lax.axis_index("grp")
    t = lax.axis_index("tile")
    z, p = t // planes, t % planes
    tok, _ = xa.shape
    ct = buf.shape[-1]
    cbuf, rbuf = buf.at[pl.ds(0, total)], buf.at[pl.ds(total, total)]
    rh = ct // 2
    xs = (xa, xm)
    is_line = g == LINE
    line_half = pl.ds(LINE * rh, rh)
    my_half = pl.ds(pl.multiple_of(g * rh, rh), rh)

    fwd = (ring_place(p) - ring_place(z) + planes) % planes
    bwd = (planes - fwd) % planes
    is_root = fwd == 0
    ring_fwd = ring_place((ring_place(p) + 1) % planes)
    ring_bwd = ring_place((ring_place(p) + planes - 1) % planes)
    fwd_is_near = ring_fwd == piece_of(p, 1)

    low_side = z < lines // 2
    upper = z // (lines // 2)
    end_z = upper * (lines - 1)
    at_end = z == end_z
    place = p + upper * (planes - 1 - 2 * p)
    beside = 1 + upper * (lines - 3)
    across = end_z + beside - z
    end_step = 2 * upper - 1
    toward = jnp.where(low_side, group, group + side)
    away = group + group + side - toward

    def crosses(turn):
        return (turn >= 1) & (turn <= 2) & ((place == 0) | (place == turn))

    def comes_late(turn, dist):
        return at_end & (dist == 1) & (turn >= 1) & (turn <= 2) & (place == turn)

    slot_late = at_end & ((place == 1) | (place == 2))

    def near_of(turn):
        return turn + 1 - 2 * (turn % 2)

    def far_of(turn):
        return (turn + 2) % planes

    def local_turn(turn):
        return jnp.where(
            is_root, turn, jnp.where(
                z == piece_of(p, 1), near_of(turn), jnp.where(z == piece_of(p, 2), far_of(turn), planes - 1 - turn)))

    def next_turn(turn, way):
        return jnp.where(fwd_is_near == (way == 0), near_of(turn), far_of(turn))

    def chip(zz, pp, gg):
        return (gg, zz * planes + pp)

    pair = chip(z, p, 1 - g)
    ring_next = [chip(z, ring_fwd, RING), chip(z, ring_bwd, RING)]

    def landed(ref, sem):
        pltpu.make_async_copy(ref, ref, sem).wait()

    def cols(block):
        return pl.ds(pl.multiple_of(block * ct, ct), ct)

    def own_index(a, turn, gg):
        return 2 * planes * a + 2 * turn + gg

    def loan_index(a, turn, gg):
        return (2 * gg + a) * (planes - 1) + turn - 1

    def load_own(a):
        return pltpu.make_async_copy(xs[a].at[:, cols(p)], cbuf.at[own_index(a, 0, g)], own_sem.at[a])

    def load(a, turn):
        return pltpu.make_async_copy(
            xs[a].at[:, cols(piece_of(p, turn))], xbuf.at[loan_index(a, turn, g)], ld_sem.at[a, turn - 1])

    for a in range(2):
        load_own(a).start()
    for turn in range(1, planes):
        for a in range(2):
            load(a, turn).start()

    barrier = pltpu.get_barrier_semaphore()

    def greet(device):
        pl.semaphore_signal(barrier, inc=1, device_id=device, device_id_type=MESH)

    greet(pair)

    @pl.when(is_line)
    def _():
        for turn in range(1, planes):
            for gg in range(2):
                greet(chip(z, piece_of(p, turn), gg))
        for turn in range(1, 3):
            @pl.when(crosses(turn))
            def _():
                greet(chip(across, piece_of(p, turn), LINE))

        @pl.when(z > 0)
        def _():
            greet(chip(z - 1, p, LINE))

        @pl.when(z < lines - 1)
        def _():
            greet(chip(z + 1, p, LINE))

        pl.semaphore_wait(
            barrier, planes + 2 + jnp.where(z > 0, 1, 0) + jnp.where(z < lines - 1, 1, 0)
            + jnp.where(crosses(1), 1, 0) + jnp.where(crosses(2), 1, 0))

    @pl.when(~is_line)
    def _():
        for device in ring_next:
            greet(device)
        for chip_next in (ring_fwd, ring_bwd):
            greet(chip(z, chip_next, LINE))
        pl.semaphore_wait(barrier, planes + 2)

    def remote(src, dst, send_sem, recv_sem, device):
        return pltpu.make_async_remote_copy(
            src_ref=src, dst_ref=dst, send_sem=send_sem, recv_sem=recv_sem, device_id=device, device_id_type=MESH)

    def s1_copy(a, turn):
        n = own_index(a, turn, g)
        return remote(xbuf.at[loan_index(a, turn, g)], cbuf.at[n], s1_send.at[a, turn - 1], c_recv.at[n],
                      chip(z, piece_of(p, turn), LINE))

    def lend_copy(a, turn):
        n = loan_index(a, turn, RING)
        return remote(xbuf.at[n], xbuf.at[n], x_send.at[a, RING, turn - 1], x_recv.at[a, turn - 1], chip(z, p, LINE))

    def cross_copy(a, turn, gg):
        n = toward + own_index(a, turn, gg)
        return remote(xbuf.at[loan_index(a, turn, gg)], cbuf.at[n], x_send.at[a, gg, turn - 1], c_recv.at[n],
                      chip(end_z, piece_of(p, turn), LINE))

    def line_copy(n, to, zz, sem):
        return remote(cbuf.at[n], cbuf.at[to], sem, c_recv.at[to], chip(zz, p, LINE))

    def pair_copy(n, sem):
        return remote(cbuf.at[n], cbuf.at[n], sem, c_recv.at[n], pair)

    def ring_copy(buf, n, to, way, sem):
        return remote(buf.at[n], rbuf.at[to], sem, r_recv.at[to], ring_next[way])

    def share_copy(n, sem):
        rows = rbuf.at[n, :, line_half]
        return remote(rows, rows, sem, r_recv.at[n], pair)

    def spot(dist, near):
        from_high = low_side == near
        inside = jnp.where(from_high, z + dist < lines, z >= dist)
        sd = jnp.where((dist == 0) | from_high, dist, dist + lines - 1)
        return sd, inside & (dist < lines)

    def drain(count, sem, buf):
        ref = buf.at[pl.ds(0, count)]
        pltpu.make_async_copy(ref, ref, sem).wait()

    def feed(sd, a, turn, gg):
        way = (turn + gg) % 2
        base = group * sd
        to = base + own_index(a, next_turn(turn, way), gg)

        @pl.when(is_root)
        def _():
            ring_copy(cbuf, base + own_index(a, turn, gg), to, way, f_send.at[sd, turn]).start()

    def col_turn(sd, turn, dist, near):
        for a in range(2):
            for gg in (LINE, RING):
                n = group * sd + own_index(a, turn, gg)

                def one(n=n, gg=gg):
                    landed(cbuf.at[n], c_recv.at[n])
                    if near is None or near is False:
                        main_ok = True
                    else:
                        main_ok = ~at_end
                    if dist is None:
                        if turn in (1, 2):
                            main_ok = main_ok & ~crosses(turn)
                        line_copy(n, n + away, z - end_step, z_send.at[2 * lines - 1, turn]).start()
                        to, zz = n + toward, z + end_step
                    else:
                        to, zz = n + group, z + (end_step if near else -end_step)

                    def main():
                        line_copy(n, to, zz, z_send.at[sd, turn]).start()

                    if main_ok is True:
                        main()
                    else:
                        pl.when(main_ok)(main)
                    feed(sd, a, turn, gg)
                    if not (dist is None and turn == 0 and gg == RING):
                        pair_copy(n, d_send.at[sd, turn]).start()

                if not (dist is None and turn == 0 and gg == LINE):
                    one()

    def row_turn(way, passes):
        def action(sd, turn, dist, near):
            here = local_turn(turn)
            gg = (turn + way) % 2
            n = group * sd + own_index(0, here, gg)
            to = group * sd + own_index(0, next_turn(here, way), gg)
            for a in range(2):
                m, to_m = n + own_index(a, 0, 0), to + own_index(a, 0, 0)
                landed(rbuf.at[m], r_recv.at[m])
                if passes:
                    ring_copy(rbuf, m, to_m, way, z_send.at[sd, turn]).start()
                share_copy(m, d_send.at[sd, turn]).start()

        return action

    def gather_waits(base, skip_own):
        @pl.when(is_line & ~is_root)
        def _():
            for j in range(2 * planes):
                landed(rbuf.at[base + j, :, line_half], r_recv.at[base + j])

        @pl.when(~is_line)
        def _():
            for j in range(2 * planes):
                if not (skip_own and j == RING):
                    landed(cbuf.at[base + j], c_recv.at[base + j])

    rows_from = jnp.where(is_root, 0, total)

    def multiply(sd, skip_own=False):
        def one(a, carry):
            base = group * sd + own_index(a, 0, 0)
            gather_waits(base, skip_own)
            lhs = buf[pl.ds(base + rows_from, 2 * planes), :, my_half].reshape(2 * planes * tok, rh)
            rhs = buf[pl.ds(base, 2 * planes)].reshape(2 * planes * tok, ct)
            out[a] += lax.dot_general(lhs, rhs, (((0,), (0,)), ((), ())), preferred_element_type=jnp.float32)
            return carry

        lax.fori_loop(0, 2, one, 0)

    for a in range(2):
        load_own(a).wait()

        @pl.when(is_line)
        def _():
            n = own_index(a, 0, LINE)

            @pl.when(~at_end)
            def _():
                line_copy(n, n + toward, z + end_step, z_send.at[0, 0]).start()
            line_copy(n, n + away, z - end_step, z_send.at[2 * lines - 1, 0]).start()
            feed(0, a, 0, LINE)
            pair_copy(n, d_send.at[0, 0]).start()

        @pl.when(~is_line)
        def _():
            pair_copy(own_index(a, 0, RING), x_send.at[a, LINE, 0]).start()

    for turn in range(1, planes):
        for a in range(2):
            load(a, turn).wait()
            s1_copy(a, turn).start()
    for turn in range(1, 3):
        @pl.when(~is_line & ~at_end & crosses(turn))
        def _():
            for a in range(2):
                lend_copy(a, turn).start()
    for a in range(2):
        out[a] = jnp.zeros_like(out[a])

    def send_cross(a, turn):
        cross_copy(a, turn, LINE).start()
        landed(xbuf.at[loan_index(a, turn, RING)], x_recv.at[a, turn - 1])
        cross_copy(a, turn, RING).start()

    def turns(block, r, shift, action):
        first = r - shift

        @pl.when(block + first // planes == 0)
        def _():
            action(0, first % planes, None, True)

        def along(near, u0, keep):
            dist = block + u0 // planes
            turn = u0 % planes
            sd, inside = spot(dist, near)

            @pl.when(inside & (dist > 0) & keep(dist, turn))
            def _():
                action(sd, turn, dist, near)

        along(True, r - shift + AHEAD, lambda dist, turn: ~at_end | (dist != 1) if turn in (1, 2) else True)
        along(False, r - shift - FAR_LAG + AHEAD, lambda dist, turn: True)
        u_x = planes + 1 + r - shift - CROSS_WAIT
        if u_x % planes in (1, 2):
            late = place == u_x % planes
            along(True, u_x, lambda dist, turn: at_end & (dist == 1) & ~(late & is_col(action)))

    def is_col(action):
        return action is col_turn

    def block_steps(block, carry):
        for r in range(planes):
            @pl.when(is_line)
            def _():
                if r == CROSS_AT % planes:
                    @pl.when((block == CROSS_AT // planes) & ~at_end)
                    def _():
                        for turn in range(1, 3):
                            @pl.when(place == turn)
                            def _():
                                for a in range(2):
                                    send_cross(a, turn)
                if r == CROSS_LATE % planes:
                    @pl.when((block == CROSS_LATE // planes) & ~at_end & (place == 0))
                    def _():
                        for a in range(2):
                            for turn in range(1, 3):
                                send_cross(a, turn)
                turns(block, r, 0, col_turn)

            @pl.when(~is_line & ~is_root)
            def _():
                @pl.when(fwd < planes - 1)
                def _():
                    turns(block, r, 0, row_turn(0, True))

                @pl.when(bwd < planes - 1)
                def _():
                    turns(block, r, 0, row_turn(1, True))

                @pl.when(fwd == planes - 1)
                def _():
                    turns(block, r, SPAN_LAG, row_turn(0, False))

                @pl.when(bwd == planes - 1)
                def _():
                    turns(block, r, SPAN_LAG, row_turn(1, False))

            if r == LATE_AT % planes:
                @pl.when(slot_late & is_line & (block == LATE_AT // planes))
                def _():
                    for a in range(2):
                        for gg in (LINE, RING):
                            n = toward + own_index(a, place, gg)
                            landed(cbuf.at[n], c_recv.at[n])
                            pair_copy(n, d_send.at[toward // group, place]).start()

            at = r - MUL_LAG
            if (at - (planes - 1)) % planes == 0:
                @pl.when(block == (planes - 1 - at) // planes)
                def _():
                    multiply(0, True)
            for near, shift in ((True, 0), (False, FAR_LAG)):
                u0 = at - shift + AHEAD
                if u0 % planes == planes - 1:
                    dist = block + u0 // planes
                    sd, inside = spot(dist, near)

                    @pl.when(inside & (dist > 0) & ~(at_end & (dist == 1)))
                    def _():
                        multiply(sd)
            u0 = planes + 1 + at - CROSS_WAIT
            if u0 % planes == 2:
                @pl.when(at_end & ~slot_late & (block + u0 // planes == 1))
                def _():
                    multiply(toward // group)
        return carry

    steps = planes * lines - AHEAD + FAR_LAG + MUL_LAG
    lax.fori_loop(0, (steps + planes - 1) // planes, block_steps, 0)

    def done(j, carry):
        dist = j % lines
        near = j < lines
        sd, inside = spot(dist, near)

        @pl.when(inside & (near | (dist > 0)))
        def _():
            for turn in range(planes):
                @pl.when(is_line)
                def _():
                    @pl.when(is_root)
                    def _():
                        drain(4, f_send.at[sd, turn], cbuf)

                    @pl.when(jnp.logical_not(near) | (~at_end & ~((dist == 0) & crosses(turn))))
                    def _():
                        drain(4, z_send.at[sd, turn], cbuf)

                    @pl.when(dist == 0)
                    def _():
                        drain(4, z_send.at[2 * lines - 1, turn], cbuf)
                    if turn == 0:
                        @pl.when(dist == 0)
                        def _():
                            drain(2, d_send.at[sd, turn], cbuf)

                        @pl.when(dist > 0)
                        def _():
                            drain(4, d_send.at[sd, turn], cbuf)
                    else:
                        drain(4, d_send.at[sd, turn], cbuf)

                @pl.when(~is_line)
                def _():
                    @pl.when(fwd == 2)
                    def _():
                        drain(4, z_send.at[sd, turn], cbuf)

                    @pl.when(~is_root & (fwd != 2))
                    def _():
                        drain(2, z_send.at[sd, turn], cbuf)

                    @pl.when(~is_root)
                    def _():
                        rows = rbuf.at[pl.ds(0, 4), :, line_half]
                        pltpu.make_async_copy(rows, rows, d_send.at[sd, turn]).wait()
        return carry

    lax.fori_loop(0, 2 * lines, done, 0)
    for turn in range(1, planes):
        for a in range(2):
            s1_copy(a, turn).wait_send()
    for a in range(2):
        @pl.when(~is_line)
        def _():
            pair_copy(own_index(a, 0, RING), x_send.at[a, LINE, 0]).wait_send()
        for turn in range(1, 3):
            @pl.when(is_line & ~at_end & crosses(turn))
            def _():
                for gg in range(2):
                    cross_copy(a, turn, gg).wait_send()

            @pl.when(~is_line & ~at_end & crosses(turn))
            def _():
                lend_copy(a, turn).wait_send()

    @pl.when(slot_late)
    def _():
        multiply(toward // group)


def fused(attn_input, mlp_input):
    groups, tiles = lax.axis_size("grp"), lax.axis_size("tile")
    tok, width = attn_input.shape
    ct, rh = width // ROWB, width // ROWB // groups
    norm_factor = 2.0 / (tok * tiles * groups)
    dma = pltpu.SemaphoreType.DMA
    group = 4 * ROWB
    total = group * (2 * ROWB - 1)
    hess = pl.pallas_call(
        kernel,
        out_shape=jax.ShapeDtypeStruct((2, rh, ct), jnp.float32),
        in_specs=[pl.BlockSpec(memory_space=IN_SPACE)] * 2,
        out_specs=pl.BlockSpec(memory_space=pltpu.VMEM),
        scratch_shapes=[
            pltpu.VMEM((4 * (ROWB - 1), tok, ct), jnp.bfloat16),
            pltpu.VMEM((2 * total, tok, ct), jnp.bfloat16),
            dma((2,)), dma((2, ROWB - 1)), dma((2, 2)), dma((total,)), dma((total,)),
            dma((2, ROWB - 1)), dma((2, groups, 2)), dma((2 * ROWB - 1, ROWB)), dma((2 * ROWB, ROWB)),
            dma((2 * ROWB - 1, ROWB)),
        ],
        compiler_params=pltpu.CompilerParams(collective_id=0, has_side_effects=True, vmem_limit_bytes=VMEM_LIMIT),
    )(pltpu.with_memory_space_constraint(attn_input, pltpu.HBM), pltpu.with_memory_space_constraint(mlp_input, pltpu.HBM))
    return hess[0][None] * norm_factor, hess[1][None] * norm_factor


def body(attn_input, mlp_input):
    if lax.axis_size("grp") == 2 and lax.axis_size("tile") == ROWB * ROWB:
        return fused(attn_input, mlp_input)
    return (hessian_share(attn_input), hessian_share(mlp_input))


def solution(mesh):
    in_specs = (P(("grp", "tile"), None), P(("grp", "tile"), None))
    out_specs = (P("tile", "grp", None), P("tile", "grp", None))
    return jax.shard_map(body, mesh=mesh, in_specs=in_specs, out_specs=out_specs, check_vma=False)
```
